32 devices in a mesh: row: 4 (over x, core), col: 8 (over z, y).
Axes of the slice: x: 2, y: 2, z: 4, core: 2. Of those that a mesh axis runs over, the one named last changes fastest.
Arguments:
- w_rec: bfloat16 [2, 4096, 4, 4096], P(None, 'row', None, 'col'), may hold values from -0.09375 to 0.09375
- w_in: bfloat16 [2, 4096, 4, 4096], P(None, 'row', None, 'col'), may hold values from -0.09375 to 0.09375
- gate_pre: float32 [2, 6, 64, 4, 4096], P(None, None, None, None, 'col'), may hold values from -8 to 8, as said below
- cells: float32 [2, 7, 64, 4096], P(None, None, None, 'col'), may hold values from -6 to 6
- layer_in: bfloat16 [2, 6, 64, 4096], P(None, None, None, 'row'), may hold values from -1 to 1
- h_prev: bfloat16 [2, 6, 64, 4096], P(None, None, None, 'row'), may hold values from -1 to 1
- top_grad: float32 [6, 64, 4096], P(None, None, 'col'), may hold values from -40 to 40
Outputs:
- w_rec_grad: bfloat16 [2, 4096, 4, 4096], P(None, 'row', None, 'col')
- w_in_grad: bfloat16 [2, 4096, 4, 4096], P(None, 'row', None, 'col')
- input_grad: float32 [6, 64, 4096], P(None, None, 'col')
The draws below stay inside these ranges and needn't reach their ends.
Inputs may be any that keep to these rules, and one draw needn't show every extreme that they name: `gate_pre`: dimension 3 holds the input, forget, candidate and output gates in that order.
All inputs are finite; a program needn't handle non-finite values.
Results may differ from the reference program's by a relative error of at most 0.0051.
Values sent between devices are 32-bit elements; how exact they have to be, the bound alone decides.
A program may use at most 128 MiB of HBM per device.

```python
import math
import jax
import jax.numpy as jnp
from jax import lax

WIDTH = 4096
LAYERS = 2
STEPS = 6
BATCH = 64


def draw_gate_pre(key, part):
    first, second = jax.random.split(jax.random.fold_in(key, 11), 2)
    shape = (LAYERS, STEPS, BATCH, 4, WIDTH)
    noise = jax.random.normal(first, shape, jnp.float32)
    offset = jax.random.uniform(second, (LAYERS, 1, 1, 1, WIDTH), jnp.float32, -1.0, 5.0)
    chosen = (jnp.arange(4) == 1).reshape(1, 1, 1, 4, 1)
    values = jnp.where(chosen, offset + 0.7 * noise, 1.5 * noise)
    return jnp.clip(values, -8.0, 8.0)


def draw_top_grad(key, part):
    first, second, third = jax.random.split(jax.random.fold_in(key, 23), 3)
    shape = (STEPS, BATCH, WIDTH)
    phases = jax.random.uniform(first, (2,), jnp.float32, 0.0, 2.0 * math.pi)
    where_unit = jnp.arange(WIDTH).astype(jnp.float32) / WIDTH
    envelope = 1.2 * jnp.sin(2.0 * math.pi * where_unit + phases[0]) + 0.6 * jnp.sin(6.0 * math.pi * where_unit + phases[1])
    factor = 2.0 * jnp.exp(envelope)
    base = jax.random.normal(second, shape, jnp.float32)
    return jnp.clip(base * factor, -40.0, 40.0)


def steps_of(rng, shape, shards, smallest, largest):
    level = 1.0
    for axis_at, blocks in shards:
        heights = jax.random.uniform(jax.random.fold_in(jax.random.fold_in(rng, 6), axis_at), (blocks,), jnp.float32, smallest / len(shards), largest / len(shards))
        level = level * jnp.repeat(jnp.exp(heights), shape[axis_at] // blocks).reshape((-1,) + (1,) * (len(shape) - 1 - axis_at))
    return level


def scatter_about(stream_key, extent, deviation, bound, shards=(), kind=jnp.bfloat16):
    array = deviation * jax.random.normal(stream_key, extent, jnp.float32)
    if shards:
        array = array * steps_of(stream_key, extent, shards, -0.22, 0.18)
    return jnp.clip(array, -bound, bound).astype(kind)


def setup_inputs(seed: int = 0) -> dict:
    streams_of = jax.random.split(jax.random.key(seed), 8)
    return {
        "w_rec": scatter_about(streams_of[0], (LAYERS, WIDTH, 4, WIDTH), WIDTH ** -0.5, 0.09375, ((1, 4), (3, 8))),
        "w_in": scatter_about(streams_of[1], (LAYERS, WIDTH, 4, WIDTH), WIDTH ** -0.5, 0.09375, ((1, 4), (3, 8))),
        "gate_pre": draw_gate_pre(jax.random.fold_in(streams_of[7], 71), 0),
        "cells": scatter_about(streams_of[3], (LAYERS, STEPS + 1, BATCH, WIDTH), 1.0, 6.0, ((3, 8),), jnp.float32),
        "layer_in": jnp.clip(jax.random.uniform(streams_of[4], (LAYERS, STEPS, BATCH, WIDTH), jnp.float32, -1.0, 1.0) * steps_of(streams_of[4], (LAYERS, STEPS, BATCH, WIDTH), ((3, 4),), -0.4, 0.0), -1.0, 1.0).astype(jnp.bfloat16),
        "h_prev": jnp.clip(jax.random.uniform(streams_of[5], (LAYERS, STEPS, BATCH, WIDTH), jnp.float32, -1.0, 1.0) * steps_of(streams_of[5], (LAYERS, STEPS, BATCH, WIDTH), ((3, 4),), -0.4, 0.0), -1.0, 1.0).astype(jnp.bfloat16),
        "top_grad": draw_top_grad(jax.random.fold_in(streams_of[7], 71), 0),
    }


def cell_backward(preact, cell_prev, cell_now, hid_grad, cell_carry):
    in_gate = jax.nn.sigmoid(preact[:, 0])
    forget = jax.nn.sigmoid(preact[:, 1])
    cand_gate = jnp.tanh(preact[:, 2])
    out_gate = jax.nn.sigmoid(preact[:, 3])
    tanh_cell = jnp.tanh(cell_now)
    cell_grad = cell_carry + hid_grad * out_gate * (1.0 - tanh_cell * tanh_cell)
    grad_in = cell_grad * cand_gate * in_gate * (1.0 - in_gate)
    grad_forget = cell_grad * cell_prev * forget * (1.0 - forget)
    grad_cand = cell_grad * in_gate * (1.0 - cand_gate * cand_gate)
    grad_out = hid_grad * tanh_cell * out_gate * (1.0 - out_gate)
    gate_grads = jnp.stack([grad_in, grad_forget, grad_cand, grad_out], axis=1).astype(jnp.bfloat16)
    return (gate_grads, cell_grad * forget)

def reference(w_rec, w_in, gate_pre, cells, layer_in, h_prev, top_grad):
    incoming = top_grad
    rec_grads = [None] * LAYERS
    in_grads = [None] * LAYERS
    sumsq = jnp.zeros((), jnp.float32)
    for layer in range(LAYERS - 1, -1, -1):
        rec_flat = w_rec[layer].reshape(WIDTH, 4 * WIDTH)

        def advance(carry, inputs, rec_flat=rec_flat):
            rec_carry, cell_carry = carry
            preact, cell_prev, cell_now, outside = inputs
            gate_grads, cell_next = cell_backward(preact, cell_prev, cell_now, outside + rec_carry, cell_carry)
            recurrent = jnp.dot(gate_grads.reshape(BATCH, 4 * WIDTH), rec_flat.T, preferred_element_type=jnp.float32)
            return ((recurrent, cell_next), gate_grads)
        zeros = jnp.zeros((BATCH, WIDTH), jnp.float32)
        carried, stacked = lax.scan(advance, (zeros, zeros), (gate_pre[layer], cells[layer, :STEPS], cells[layer, 1:], incoming), reverse=True)
        flat = stacked.reshape(STEPS * BATCH, 4 * WIDTH)
        incoming = jnp.dot(flat, w_in[layer].reshape(WIDTH, 4 * WIDTH).T, preferred_element_type=jnp.float32).reshape(STEPS, BATCH, WIDTH)
        raw_rec = jnp.dot(h_prev[layer].reshape(STEPS * BATCH, WIDTH).T, flat, preferred_element_type=jnp.float32)
        raw_in = jnp.dot(layer_in[layer].reshape(STEPS * BATCH, WIDTH).T, flat, preferred_element_type=jnp.float32)
        sumsq = sumsq + jnp.sum(raw_rec * raw_rec) + jnp.sum(raw_in * raw_in)
        rec_grads[layer] = raw_rec
        in_grads[layer] = raw_in
    scale = 1.0 / jnp.maximum(jnp.sqrt(sumsq / (8.0 * LAYERS * WIDTH * WIDTH)), 0.05)
    w_rec_grad = jnp.stack([(rec_grads[layer] * scale).reshape(WIDTH, 4, WIDTH) for layer in range(LAYERS)]).astype(jnp.bfloat16)
    w_in_grad = jnp.stack([(in_grads[layer] * scale).reshape(WIDTH, 4, WIDTH) for layer in range(LAYERS)]).astype(jnp.bfloat16)
    return (w_rec_grad, w_in_grad, incoming)
```

```python
import functools

import jax
import jax.numpy as jnp
from jax import lax
from jax.experimental import pallas as pl
from jax.experimental.pallas import tpu as pltpu
from jax.sharding import PartitionSpec as P

MESH = pl.DeviceIdType.MESH


def split_col(cols, ratio):
    fast = 1
    while fast * fast * 2 <= cols:
        fast *= 2
    while fast < ratio:
        fast *= 2
    return cols // fast, fast


def exchange_kernel(blocks, rows, cols, scalar, *refs):
    ratio = cols // rows
    slow_n, fast_n = split_col(cols, ratio)
    per = fast_n // ratio
    parts, refs = refs[:blocks], refs[blocks:]
    if scalar:
        sq_in, out, sq_out = refs[:3]
        refs = refs[3:]
    else:
        out = refs[0]
        refs = refs[1:]
    recv1, acc1, recv2, acc2, land, s1, r1, s2, r2, s3, r3 = refs[:11]
    if scalar:
        sq1, sqa1, sq2, sqa2, sq3, qs1, qr1, qs2, qr2, qs3, qr3 = refs[11:]
    width = recv1.shape[-1]
    mini = acc2.shape[1]
    row = lax.axis_index("row")
    col = lax.axis_index("col")
    slow, fast = col // fast_n, col % fast_n
    target = ratio * row + fast // per
    is_own = target == col
    source_row = col // ratio

    def fast_peer(d):
        return slow * fast_n + (fast + d) % fast_n

    def slow_peer(d):
        return ((slow + d) % slow_n) * fast_n + fast

    def source_col(z, j):
        return z * fast_n + (col % ratio) * per + j

    barrier = pltpu.get_barrier_semaphore()

    def greet(device):
        pl.semaphore_signal(barrier, inc=1, device_id=device, device_id_type=MESH)

    for d in range(1, fast_n):
        greet((row, fast_peer(d)))
    for d in range(1, slow_n):
        greet((row, slow_peer(d)))
    for z in range(slow_n):
        for j in range(per):
            other = source_col(z, j)

            @pl.when(jnp.logical_not((source_row == row) & (other == col)))
            def _(other=other):
                greet((source_row, other))

    count = fast_n - 1 + slow_n - 1 + rows - 1
    if scalar:
        for d in range(1, rows):
            greet(((row + d) % rows, col))
        count += rows - 1
    pl.semaphore_wait(barrier, count + jnp.where(is_own, 0, 1))

    def lanes(index):
        return pl.ds(pl.multiple_of(index * width, width), width)

    def subs(index):
        return pl.ds(pl.multiple_of(index * mini, mini), mini)

    def remote(src, dst, send, recv, device):
        return pltpu.make_async_remote_copy(
            src_ref=src, dst_ref=dst, send_sem=send, recv_sem=recv,
            device_id=device, device_id_type=MESH,
        )

    def copy1(b, d):
        peer = (fast + d) % fast_n
        return remote(parts[b].at[:, lanes(peer)], recv1.at[b, d - 1], s1.at[b, d - 1],
                      r1.at[b, d - 1], (row, fast_peer(d)))

    def copy2(b, d):
        peer = (slow + d) % slow_n
        return remote(acc1.at[b, subs(peer), :], recv2.at[b, d - 1], s2.at[b, d - 1],
                      r2.at[b, d - 1], (row, slow_peer(d)))

    def copy3(b, d):
        return remote(acc2.at[b], land.at[b, subs(slow), lanes(fast % per)], s3.at[b, d],
                      r3.at[b, slow * per + fast % per], ((row + d) % rows, target))

    def scalar1(d):
        return remote(sq_in, sq1.at[d - 1], qs1.at[d - 1], qr1.at[d - 1], (row, fast_peer(d)))

    def scalar2(d):
        return remote(sqa1, sq2.at[d - 1], qs2.at[d - 1], qr2.at[d - 1], (row, slow_peer(d)))

    def scalar3(d):
        return remote(sqa2, sq3.at[d - 1], qs3.at[d - 1], qr3.at[d - 1], ((row + d) % rows, col))

    if scalar:
        for d in range(1, fast_n):
            scalar1(d).start()
    for b in range(blocks):
        for d in range(1, fast_n):
            copy1(b, d).start()
    if scalar:
        value = sq_in[...]
        for d in range(1, fast_n):
            scalar1(d).wait_recv()
            value = value + sq1[d - 1]
        sqa1[...] = value
        for d in range(1, slow_n):
            scalar2(d).start()
    for b in range(blocks):
        value = parts[b][:, lanes(fast)]
        for d in range(1, fast_n):
            copy1(b, d).wait_recv()
            value = value + recv1[b, d - 1]
        acc1[b] = value
        for d in range(1, slow_n):
            copy2(b, d).start()
    if scalar:
        value = sqa1[...]
        for d in range(1, slow_n):
            scalar2(d).wait_recv()
            value = value + sq2[d - 1]
        sqa2[...] = value
        for d in range(1, rows):
            scalar3(d).start()
    for b in range(blocks):
        value = acc1[b, subs(slow), :]
        for d in range(1, slow_n):
            copy2(b, d).wait_recv()
            value = value + recv2[b, d - 1]
        acc2[b] = value

        @pl.when(is_own)
        def _(b=b, value=value):
            land[b, subs(slow), lanes(fast % per)] = value

        @pl.when(jnp.logical_not(is_own))
        def _(b=b):
            copy3(b, 0).start()

        for d in range(1, rows):
            copy3(b, d).start()
    if scalar:
        value = sqa2[...]
        for d in range(1, rows):
            scalar3(d).wait_recv()
            value = value + sq3[d - 1]
        sq_out[...] = value
    for b in range(blocks):
        for z in range(slow_n):
            for j in range(per):
                mine = (source_row == row) & (source_col(z, j) == col)

                @pl.when(jnp.logical_not(mine))
                def _(b=b, z=z, j=j):
                    spot = land.at[b, pl.ds(z * mini, mini), pl.ds(j * width, width)]
                    remote(spot, spot, s3.at[b, 0], r3.at[b, z * per + j],
                           (source_row, source_col(z, j))).wait_recv()

        out[b] = land[b]
    for b in range(blocks):
        for d in range(1, fast_n):
            copy1(b, d).wait_send()
        for d in range(1, slow_n):
            copy2(b, d).wait_send()
        for d in range(1, rows):
            copy3(b, d).wait_send()

        @pl.when(jnp.logical_not(is_own))
        def _(b=b):
            copy3(b, 0).wait_send()
    if scalar:
        for d in range(1, fast_n):
            scalar1(d).wait_send()
        for d in range(1, slow_n):
            scalar2(d).wait_send()
        for d in range(1, rows):
            scalar3(d).wait_send()


def exchange(parts, squares, collective):
    rows, cols = lax.axis_size("row"), lax.axis_size("col")
    ratio = cols // rows
    slow_n, fast_n = split_col(cols, ratio)
    blocks = len(parts)
    batch, units = parts[0].shape
    width, mini = units // fast_n, batch // slow_n
    scalar = squares is not None
    per = fast_n // ratio
    dma = pltpu.SemaphoreType.DMA
    vmem = lambda *shape: pltpu.VMEM(shape, jnp.float32)
    scratch = [
        vmem(blocks, fast_n - 1, batch, width), vmem(blocks, batch, width),
        vmem(blocks, slow_n - 1, mini, width), vmem(blocks, mini, width),
        vmem(blocks, batch, units // ratio),
        dma((blocks, fast_n - 1)), dma((blocks, fast_n - 1)),
        dma((blocks, slow_n - 1)), dma((blocks, slow_n - 1)),
        dma((blocks, rows)), dma((blocks, slow_n * per)),
    ]
    shapes = [jax.ShapeDtypeStruct((blocks, batch, units // ratio), jnp.float32)]
    args = list(parts)
    if scalar:
        args.append(squares)
        shapes.append(jax.ShapeDtypeStruct(squares.shape, jnp.float32))
        tile = squares.shape
        scratch += [
            vmem(fast_n - 1, *tile), vmem(*tile), vmem(slow_n - 1, *tile), vmem(*tile), vmem(rows - 1, *tile),
            dma((fast_n - 1,)), dma((fast_n - 1,)), dma((slow_n - 1,)), dma((slow_n - 1,)),
            dma((rows - 1,)), dma((rows - 1,)),
        ]
    in_vmem = pl.BlockSpec(memory_space=pltpu.VMEM)
    return pl.pallas_call(
        functools.partial(exchange_kernel, blocks, rows, cols, scalar),
        out_shape=shapes,
        in_specs=[in_vmem] * len(args),
        out_specs=[in_vmem] * len(shapes),
        scratch_shapes=scratch,
        compiler_params=pltpu.CompilerParams(collective_id=collective, has_side_effects=True),
        name="exchange",
    )(*args)


def cell_backward(preact, cell_prev, cell_now, hid_grad, cell_carry):
    in_gate = jax.nn.sigmoid(preact[:, 0])
    forget = jax.nn.sigmoid(preact[:, 1])
    cand_gate = jnp.tanh(preact[:, 2])
    out_gate = jax.nn.sigmoid(preact[:, 3])
    tanh_cell = jnp.tanh(cell_now)
    cell_grad = cell_carry + hid_grad * out_gate * (1.0 - tanh_cell * tanh_cell)
    grad_in = cell_grad * cand_gate * in_gate * (1.0 - in_gate)
    grad_forget = cell_grad * cell_prev * forget * (1.0 - forget)
    grad_cand = cell_grad * in_gate * (1.0 - cand_gate * cand_gate)
    grad_out = hid_grad * tanh_cell * out_gate * (1.0 - out_gate)
    gates = jnp.concatenate([grad_in, grad_forget, grad_cand, grad_out], axis=1)
    return (gates.astype(jnp.bfloat16), cell_grad * forget)


def contract(left, right, dims):
    return lax.dot_general(left, right, ((dims, dims), ((), ())), preferred_element_type=jnp.float32)


def local(w_rec, w_in, gate_pre, cells, layer_in, h_prev, top_grad):
    layers, row_units = w_rec.shape[:2]
    steps, batch, col_units = top_grad.shape
    rec_flats = [w_rec[layer].reshape(row_units, 4 * col_units) for layer in range(layers)]
    in_flats = [w_in[layer].reshape(row_units, 4 * col_units) for layer in range(layers)]
    zeros = jnp.zeros((batch, col_units), jnp.float32)
    recurrent = [zeros] * layers
    carry = [zeros] * layers
    incoming = [None] * layers
    store = [[None] * steps for _ in range(layers)]
    for diagonal in range(steps + layers - 1):
        parts, goes = [], []
        for layer in range(layers - 1, -1, -1):
            step = steps - 1 - diagonal + layers - 1 - layer
            if not 0 <= step < steps:
                continue
            outside = top_grad[step] if layer == layers - 1 else incoming[layer]
            gates, carry[layer] = cell_backward(
                gate_pre[layer, step], cells[layer, step], cells[layer, step + 1],
                outside + recurrent[layer], carry[layer],
            )
            store[layer][step] = gates
            if step > 0:
                parts.append(contract(gates, rec_flats[layer], (1,)))
                goes.append((recurrent, layer))
            if layer > 0:
                parts.append(contract(gates, in_flats[layer], (1,)))
                goes.append((incoming, layer - 1))
        if parts:
            units = exchange(parts, None, len(parts))[0]
            for index, (where, layer) in enumerate(goes):
                where[layer] = units[index]
    flats = [jnp.concatenate(store[layer], axis=0) for layer in range(layers)]
    rec_in = [h_prev[layer].reshape(steps * batch, row_units) for layer in range(layers)]
    lay_in = [layer_in[layer].reshape(steps * batch, row_units) for layer in range(layers)]
    sumsq = 0.0
    for layer in range(layers):
        inputs_gram = contract(rec_in[layer], rec_in[layer], (1,)) + contract(lay_in[layer], lay_in[layer], (1,))
        sumsq = sumsq + jnp.sum(inputs_gram * contract(flats[layer], flats[layer], (1,)))
    last = [contract(store[0][step], in_flats[0], (1,)) for step in range(steps)]
    input_grad, squares = exchange(last, jnp.broadcast_to(sumsq, (8, 128)), 0)
    entries = 2.0 * layers * (row_units * lax.axis_size("row")) * (4 * col_units * lax.axis_size("col"))
    scale = 1.0 / jnp.maximum(jnp.sqrt(squares[0, 0] / entries), 0.05)

    def weight_grad(inputs):
        return jnp.stack([
            (contract(inputs[layer], flats[layer], (0,)) * scale).astype(jnp.bfloat16)
            .reshape(row_units, 4, col_units)
            for layer in range(layers)
        ])

    return (weight_grad(rec_in), weight_grad(lay_in), input_grad)


def solution(mesh):
    placed = (
        P(None, "row", None, "col"),
        P(None, "row", None, "col"),
        P(None, None, None, None, "col"),
        P(None, None, None, "col"),
        P(None, None, None, "row"),
        P(None, None, None, "row"),
        P(None, None, "col"),
    )
    return jax.shard_map(
        local,
        mesh=mesh,
        in_specs=placed,
        out_specs=(P(None, "row", None, "col"), P(None, "row", None, "col"), P(None, None, "col")),
        check_vma=False,
    )
```
